32 devices in a mesh: modes: 8 (over z, y), cheb: 4 (over x, core).
Axes of the slice: x: 2, y: 2, z: 4, core: 2. Of those that a mesh axis runs over, the one named last changes fastest.
Arguments:
- start: float32 [2, 2, 2048, 256], P(None, None, ('modes', 'cheb')), may hold values from -45 to 45
- forcing: float32 [2, 2, 2048, 256], P(None, None, ('modes', 'cheb')), may hold values from -45 to 45
- taus: float32 [2048, 256, 256], P(('modes', 'cheb')), may hold values from -5 to 5
Outputs:
- solution: float32 [2, 2, 2048, 256], P(None, None, ('modes', 'cheb'))
The draws below stay inside these ranges and needn't reach their ends.
All inputs are finite; a program needn't handle non-finite values.
Results may differ from the reference program's by a relative error of at most 0.0002.
Values sent between devices are 32-bit elements; how exact they have to be, the bound alone decides.
A program may use at most 128 MiB of HBM per device.

```python
import math
import jax
import jax.numpy as jnp
from jax import lax

KX = 2048
NY = 256
BATCH = 2
NEWTON = 2
KRYLOV = 3


def spectral_field(key):
    subkeys = jax.random.split(key, 3)
    entries = jnp.clip(jax.random.normal(subkeys[0], (BATCH, 2, KX, NY), jnp.float32), -5.0, 5.0)
    log_low = math.log(0.3)
    log_high = math.log(3.0)
    mode_scale = jnp.exp(jax.random.uniform(subkeys[1], (1, 1, KX, 1), jnp.float32, log_low, log_high))
    degree_scale = jnp.exp(jax.random.uniform(subkeys[2], (1, 1, 1, NY), jnp.float32, log_low, log_high))
    return entries * mode_scale * degree_scale


def draw_start(key, part):
    return spectral_field(jax.random.fold_in(key, 11))


def draw_forcing(key, part):
    return spectral_field(jax.random.fold_in(key, 23))


def draw_taus(key, part):
    subkeys = jax.random.split(jax.random.fold_in(key, 37), 3)
    wavenumber = 16.0 * jnp.arange(KX, dtype=jnp.int32).astype(jnp.float32) / KX
    envelope = 1.0 / (1.0 + wavenumber * wavenumber / 16.0)
    rough = jnp.exp(jax.random.uniform(subkeys[0], (KX,), jnp.float32, math.log(0.5), math.log(2.0)))
    diagonal = jnp.exp(jax.random.uniform(subkeys[1], (KX, NY), jnp.float32, math.log(0.5), math.log(2.0)))
    offdiag = jnp.clip(jax.random.normal(subkeys[2], (KX, NY, NY), jnp.float32), -5.0, 5.0)
    matrix = offdiag * (0.3 / math.sqrt(NY)) + diagonal[:, :, None] * jnp.eye(NY, dtype=jnp.float32)[None, :, :]
    return matrix * (envelope * rough)[:, None, None]


def setup_inputs(seed: int = 0) -> dict:
    streams_of = jax.random.split(jax.random.key(seed), 4)
    return {
        "start": draw_start(jax.random.fold_in(streams_of[3], 71), 0),
        "forcing": draw_forcing(jax.random.fold_in(streams_of[3], 71), 0),
        "taus": draw_taus(jax.random.fold_in(streams_of[3], 71), 0),
    }


HIGH = lax.Precision.HIGHEST
STRENGTH = 0.1

def cheb_rows(degree_count):
    degree = jnp.arange(degree_count, dtype=jnp.int32)[:, None]
    node = 2 * jnp.arange(degree_count, dtype=jnp.int32)[None, :] + 1
    turns = degree * node % (4 * degree_count)
    return jnp.cos(2.0 * math.pi / (4 * degree_count) * turns.astype(jnp.float32))

def sample_grid(values):
    spectrum = lax.complex(values[:, 0], values[:, 1])
    spectrum = jnp.concatenate([spectrum, jnp.zeros_like(spectrum[:, :1])], axis=1)
    return jnp.fft.irfft(spectrum, n=2 * KX, axis=1) * (2 * KX / math.sqrt(KX * NY))

def to_points(coefs, cheb_table):
    values = jnp.einsum('brkn,ni->brki', coefs, cheb_table, precision=HIGH)
    wavenumber = (16.0 * jnp.arange(KX, dtype=jnp.int32).astype(jnp.float32) / KX)[:, None]
    slopes = jnp.stack([-wavenumber * values[:, 1], wavenumber * values[:, 0]], axis=1)
    return (sample_grid(values), sample_grid(slopes))

def to_coefficients(points, cheb_table):
    spectrum = jnp.fft.rfft(points, axis=1)[:, :KX] / (2 * KX)
    parts = jnp.stack([jnp.real(spectrum), jnp.imag(spectrum)], axis=1).astype(points.dtype)
    weights = (jnp.where(jnp.arange(NY) == 0, 1.0, 2.0) / NY).astype(points.dtype)
    coefs = jnp.einsum('brki,ni->brkn', parts, cheb_table, precision=HIGH)
    return coefs * weights * math.sqrt(KX * NY)

def precondition(coefs, taus):
    tau_keep = (jnp.arange(NY) < NY - 2).astype(coefs.dtype)
    return jnp.einsum('kam,brkm->brka', taus, coefs * tau_keep, precision=HIGH)

def least_squares(hessen, beta_norm):
    steps_count = len(hessen)
    matrix = [[hessen[col_index][:, row_index] for row_index in range(col_index + 2)] for col_index in range(steps_count)]
    target = [beta_norm] + [jnp.zeros_like(beta_norm) for row_index in range(steps_count)]
    cosines = []
    sines_list = []
    for col_index in range(steps_count):
        column = matrix[col_index]
        for row_index in range(col_index):
            upper_entry = cosines[row_index] * column[row_index] + sines_list[row_index] * column[row_index + 1]
            lower_entry = cosines[row_index] * column[row_index + 1] - sines_list[row_index] * column[row_index]
            column[row_index] = upper_entry
            column[row_index + 1] = lower_entry
        radius = jnp.sqrt(column[col_index] * column[col_index] + column[col_index + 1] * column[col_index + 1])
        cosines.append(column[col_index] / radius)
        sines_list.append(column[col_index + 1] / radius)
        column[col_index] = radius
        target[col_index + 1] = -sines_list[col_index] * target[col_index]
        target[col_index] = cosines[col_index] * target[col_index]
    solved = [None] * steps_count
    for row_index in reversed(range(steps_count)):
        partial_sum = target[row_index]
        for col_index in range(row_index + 1, steps_count):
            partial_sum = partial_sum - matrix[col_index][row_index] * solved[col_index]
        solved[row_index] = partial_sum / matrix[row_index][row_index]
    return solved

def reference(start, forcing, taus):
    cheb_table = cheb_rows(NY)
    iterate = start
    for newton_step in range(NEWTON):
        base_points, base_slopes = to_points(iterate, cheb_table)
        residual = iterate + precondition(to_coefficients(STRENGTH * base_points * base_slopes, cheb_table) - forcing, taus)
        beta_norm = jnp.sqrt(lax.optimization_barrier(jnp.sum(residual * residual, axis=(1, 2, 3))))
        krylov_basis = [-residual / beta_norm[:, None, None, None]]
        hessen = []
        for column in range(KRYLOV):
            probe_points, probe_slopes = to_points(krylov_basis[column], cheb_table)
            product = STRENGTH * (base_points * probe_slopes + probe_points * base_slopes)
            applied = krylov_basis[column] + precondition(to_coefficients(product, cheb_table), taus)
            projections = jnp.stack([lax.optimization_barrier(jnp.sum(vector * applied, axis=(1, 2, 3))) for vector in krylov_basis], axis=1)
            for index, vector in enumerate(krylov_basis):
                applied = applied - projections[:, index][:, None, None, None] * vector
            length = jnp.sqrt(lax.optimization_barrier(jnp.sum(applied * applied, axis=(1, 2, 3))))
            hessen.append(jnp.concatenate([projections, length[:, None]], axis=1))
            krylov_basis.append(applied / length[:, None, None, None])
        solved = least_squares(hessen, beta_norm)
        for column in range(KRYLOV):
            iterate = iterate + solved[column][:, None, None, None] * krylov_basis[column]
    return iterate
```

```python
import math

import jax
import jax.numpy as jnp
from jax import lax
from jax.sharding import PartitionSpec as P

NEWTON = 2
KRYLOV = 3


PREC = lax.Precision.HIGH
STRENGTH = 0.1
AXES = ("modes", "cheb")
STAT_LANES = 128


def cheb_rows(degree_count):
    degree = jnp.arange(degree_count, dtype=jnp.int32)[:, None]
    node = 2 * jnp.arange(degree_count, dtype=jnp.int32)[None, :] + 1
    turns = degree * node % (4 * degree_count)
    return jnp.cos(2.0 * math.pi / (4 * degree_count) * turns.astype(jnp.float32))


def phase_table(row_count, col_count, period):
    row_index = jnp.arange(row_count, dtype=jnp.int32)[:, None]
    col_index = jnp.arange(col_count, dtype=jnp.int32)[None, :]
    turns = row_index * col_index % period
    angle = 2.0 * math.pi / period * turns.astype(jnp.float32)
    return (jnp.cos(angle), jnp.sin(angle))


def least_squares(hessen, beta_norm):
    steps_count = len(hessen)
    matrix = [
        [hessen[col_index][:, row_index] for row_index in range(col_index + 2)]
        for col_index in range(steps_count)
    ]
    target = [beta_norm] + [jnp.zeros_like(beta_norm) for row_index in range(steps_count)]
    cosines = []
    sines_list = []
    for col_index in range(steps_count):
        column = matrix[col_index]
        for row_index in range(col_index):
            upper_entry = (
                cosines[row_index] * column[row_index]
                + sines_list[row_index] * column[row_index + 1]
            )
            lower_entry = (
                cosines[row_index] * column[row_index + 1]
                - sines_list[row_index] * column[row_index]
            )
            column[row_index] = upper_entry
            column[row_index + 1] = lower_entry
        radius = jnp.sqrt(
            column[col_index] * column[col_index] + column[col_index + 1] * column[col_index + 1]
        )
        cosines.append(column[col_index] / radius)
        sines_list.append(column[col_index + 1] / radius)
        column[col_index] = radius
        target[col_index + 1] = -sines_list[col_index] * target[col_index]
        target[col_index] = cosines[col_index] * target[col_index]
    solved = [None] * steps_count
    for row_index in reversed(range(steps_count)):
        partial_sum = target[row_index]
        for col_index in range(row_index + 1, steps_count):
            partial_sum = partial_sum - matrix[col_index][row_index] * solved[col_index]
        solved[row_index] = partial_sum / matrix[row_index][row_index]
    return solved


def shards(start, forcing, taus):
    group_size = lax.axis_size(AXES)
    batch, parts, local_modes, degrees = start.shape
    total_modes = local_modes * group_size
    points_count = 2 * total_modes
    outer_len = max(2 ** ((points_count.bit_length() - 1) // 2), local_modes)
    inner_len = points_count // outer_len
    half_inner = inner_len // 2
    split = outer_len // local_modes
    rows = degrees // group_size
    block_lanes = batch * 2 * local_modes
    fields = rows * batch
    spread = 1.0 / math.sqrt(total_modes * degrees)
    gather_factor = math.sqrt(total_modes * degrees) / points_count
    cheb_table = cheb_rows(degrees)
    tau_keep = (jnp.arange(degrees) < degrees - 2).astype(jnp.float32)
    coef_weights = jnp.where(jnp.arange(degrees) == 0, 1.0, 2.0).astype(jnp.float32) / degrees
    back_table = cheb_table * (coef_weights * tau_keep)[:, None]

    section_cos, section_sin = phase_table(inner_len, half_inner, inner_len)
    out_table = jnp.concatenate([section_cos, section_sin], axis=1)
    in_table = jnp.concatenate([section_cos, section_sin], axis=0).T
    twist_cos, twist_sin = phase_table(inner_len, outer_len, points_count)
    final_cos, final_sin = phase_table(outer_len, outer_len, outer_len)
    turn_cos = (
        twist_cos[:, :, None] * final_cos[None] - twist_sin[:, :, None] * final_sin[None]
    )
    turn_sin = (
        twist_sin[:, :, None] * final_cos[None] + twist_cos[:, :, None] * final_sin[None]
    )
    turn_table = lax.optimization_barrier(jnp.concatenate([turn_cos, -turn_sin], axis=1))
    mode = (
        outer_len * jnp.arange(half_inner, dtype=jnp.int32)[:, None]
        + jnp.arange(outer_len, dtype=jnp.int32)[None, :]
    )
    wavenumber = (16.0 * mode.astype(jnp.float32) / total_modes)[:, None, None, :]
    weights = (jnp.where(mode == 0, 1.0, 2.0).astype(jnp.float32) * spread)[:, None, None, :]

    def exchange(blocks):
        return lax.all_to_all(blocks, AXES, split_axis=0, concat_axis=0, tiled=True)

    def stat_block(stats):
        flat = jnp.pad(stats.reshape(-1), (0, STAT_LANES - stats.size))
        return jnp.broadcast_to(flat, (group_size, rows, STAT_LANES))

    def read_stats(received, shape):
        flat = jnp.sum(received[:, 0, :], axis=0)
        return flat[: math.prod(shape)].reshape(shape)

    def to_points(coefs, stats):
        values = jnp.einsum("ni,brkn->ibrk", cheb_table, coefs, precision=PREC)
        blocks = values.reshape(group_size, rows, block_lanes)
        if stats is not None:
            blocks = jnp.concatenate([blocks, stat_block(stats)], axis=2)
        received = exchange(blocks)
        summed = None
        if stats is not None:
            summed = read_stats(received[:, :, block_lanes:], stats.shape)
            received = received[:, :, :block_lanes]
        spectrum = received.reshape(half_inner, split, rows, batch, 2, local_modes)
        spectrum = spectrum.transpose(0, 2, 3, 4, 1, 5).reshape(
            half_inner, fields, 2, outer_len
        )
        real = spectrum[:, :, :1] * weights
        imag = spectrum[:, :, 1:] * weights
        slope_real = -wavenumber * imag
        slope_imag = wavenumber * real
        upper = jnp.concatenate([real, imag, slope_real, slope_imag], axis=2)
        lower = jnp.concatenate([-imag, real, -slope_imag, slope_real], axis=2)
        stacked = jnp.concatenate([upper, lower], axis=0).reshape(2 * half_inner, -1)
        turned = jnp.dot(out_table, stacked, precision=PREC)
        turned = turned.reshape(inner_len, fields * 2, 2 * outer_len)
        points = jnp.einsum("jya,jat->jyt", turned, turn_table, precision=PREC)
        return points.reshape(inner_len, rows, batch, 2, outer_len), summed

    def to_coefficients(points):
        flat = points.reshape(inner_len, fields, outer_len)
        turned = jnp.einsum("jyt,jat->jya", flat, turn_table, precision=PREC) * gather_factor
        real = turned[:, :, :outer_len]
        imag = turned[:, :, outer_len:]
        stacked = jnp.concatenate(
            [turned, jnp.concatenate([imag, -real], axis=2)], axis=0
        ).reshape(2 * inner_len, -1)
        spectrum = jnp.dot(in_table, stacked, precision=PREC)
        blocks = spectrum.reshape(half_inner, rows, batch, 2, split, local_modes)
        blocks = blocks.transpose(0, 4, 1, 2, 3, 5).reshape(group_size, rows, block_lanes)
        received = exchange(blocks).reshape(degrees, batch, 2, local_modes)
        return jnp.einsum("ibrk,ni->brkn", received, back_table, precision=PREC)

    def precondition(coefs):
        return jnp.einsum("kam,brkm->brka", taus, coefs, precision=PREC)

    def on_points(scale):
        return scale[None, None, :, None, None]

    def on_coefs(scale):
        return scale[:, None, None, None]

    iterate = start
    kept_forcing = forcing * tau_keep
    base, nothing = to_points(iterate, None)
    for newton_step in range(NEWTON):
        base_points, base_slopes = base[:, :, :, 0], base[:, :, :, 1]
        residual = iterate + precondition(
            to_coefficients(STRENGTH * base_points * base_slopes) - kept_forcing
        )
        local_square = jnp.sum(residual * residual, axis=(1, 2, 3))
        image, squared = to_points(residual, local_square)
        beta_norm = jnp.sqrt(squared)
        krylov_basis = [-residual / on_coefs(beta_norm)]
        images = [-image / on_points(beta_norm)]
        hessen = []
        for column in range(KRYLOV):
            probe_points, probe_slopes = images[column][:, :, :, 0], images[column][:, :, :, 1]
            product = STRENGTH * (base_points * probe_slopes + probe_points * base_slopes)
            applied = krylov_basis[column] + precondition(to_coefficients(product))
            local_stats = jnp.stack(
                [jnp.sum(vector * applied, axis=(1, 2, 3)) for vector in krylov_basis + [applied]],
                axis=1,
            )
            last = column == KRYLOV - 1
            if last:
                stats = read_stats(exchange(stat_block(local_stats)), local_stats.shape)
            else:
                image, stats = to_points(applied, local_stats)
            projections, square = stats[:, :-1], stats[:, -1]
            length = jnp.sqrt(square - jnp.sum(projections * projections, axis=1))
            hessen.append(jnp.concatenate([projections, length[:, None]], axis=1))
            if not last:
                for index in range(column + 1):
                    applied = applied - on_coefs(projections[:, index]) * krylov_basis[index]
                    image = image - on_points(projections[:, index]) * images[index]
                krylov_basis.append(applied / on_coefs(length))
                images.append(image / on_points(length))
        solved = least_squares(hessen, beta_norm)
        for column in range(KRYLOV):
            iterate = iterate + on_coefs(solved[column]) * krylov_basis[column]
            base = base + on_points(solved[column]) * images[column]
    return iterate


def solution(mesh):
    return jax.shard_map(
        shards,
        mesh=mesh,
        in_specs=(
            P(None, None, ("modes", "cheb"), None),
            P(None, None, ("modes", "cheb"), None),
            P(("modes", "cheb"), None, None),
        ),
        out_specs=P(None, None, ("modes", "cheb"), None),
        check_vma=False,
    )
```

```python
import math

import jax
import jax.numpy as jnp
from jax import lax
from jax.sharding import PartitionSpec as P

NEWTON = 2
KRYLOV = 3


PREC = lax.Precision.HIGH
STRENGTH = 0.1
AXES = ("modes", "cheb")
STAT_LANES = 128


def cheb_rows(degree_count):
    degree = jnp.arange(degree_count, dtype=jnp.int32)[:, None]
    node = 2 * jnp.arange(degree_count, dtype=jnp.int32)[None, :] + 1
    turns = degree * node % (4 * degree_count)
    return jnp.cos(2.0 * math.pi / (4 * degree_count) * turns.astype(jnp.float32))


def phase_table(row_count, col_count, period):
    row_index = jnp.arange(row_count, dtype=jnp.int32)[:, None]
    col_index = jnp.arange(col_count, dtype=jnp.int32)[None, :]
    turns = row_index * col_index % period
    angle = 2.0 * math.pi / period * turns.astype(jnp.float32)
    return (jnp.cos(angle), jnp.sin(angle))


def least_squares(hessen, beta_norm):
    steps_count = len(hessen)
    matrix = [
        [hessen[col_index][:, row_index] for row_index in range(col_index + 2)]
        for col_index in range(steps_count)
    ]
    target = [beta_norm] + [jnp.zeros_like(beta_norm) for row_index in range(steps_count)]
    cosines = []
    sines_list = []
    for col_index in range(steps_count):
        column = matrix[col_index]
        for row_index in range(col_index):
            upper_entry = (
                cosines[row_index] * column[row_index]
                + sines_list[row_index] * column[row_index + 1]
            )
            lower_entry = (
                cosines[row_index] * column[row_index + 1]
                - sines_list[row_index] * column[row_index]
            )
            column[row_index] = upper_entry
            column[row_index + 1] = lower_entry
        radius = jnp.sqrt(
            column[col_index] * column[col_index] + column[col_index + 1] * column[col_index + 1]
        )
        cosines.append(column[col_index] / radius)
        sines_list.append(column[col_index + 1] / radius)
        column[col_index] = radius
        target[col_index + 1] = -sines_list[col_index] * target[col_index]
        target[col_index] = cosines[col_index] * target[col_index]
    solved = [None] * steps_count
    for row_index in reversed(range(steps_count)):
        partial_sum = target[row_index]
        for col_index in range(row_index + 1, steps_count):
            partial_sum = partial_sum - matrix[col_index][row_index] * solved[col_index]
        solved[row_index] = partial_sum / matrix[row_index][row_index]
    return solved


def shards(start, forcing, taus):
    group_size = lax.axis_size(AXES)
    batch, parts, local_modes, degrees = start.shape
    total_modes = local_modes * group_size
    points_count = 2 * total_modes
    outer_len = max(2 ** ((points_count.bit_length() - 1) // 2), local_modes)
    inner_len = points_count // outer_len
    half_inner = inner_len // 2
    split = outer_len // local_modes
    rows = degrees // group_size
    block_lanes = batch * 2 * local_modes
    fields = rows * batch
    spread = 1.0 / math.sqrt(total_modes * degrees)
    gather_factor = math.sqrt(total_modes * degrees) / points_count
    cheb_table = cheb_rows(degrees)
    tau_keep = (jnp.arange(degrees) < degrees - 2).astype(jnp.float32)
    coef_weights = jnp.where(jnp.arange(degrees) == 0, 1.0, 2.0).astype(jnp.float32) / degrees
    back_table = cheb_table * (coef_weights * tau_keep)[:, None]

    section_cos, section_sin = phase_table(inner_len, half_inner, inner_len)
    value_table = jnp.stack([section_cos, section_sin])
    slope_table = jnp.stack([-section_sin, section_cos])
    back_cos, back_sin = section_cos.T, section_sin.T
    twist_cos, twist_sin = phase_table(inner_len, outer_len, points_count)
    final_cos, final_sin = phase_table(outer_len, outer_len, outer_len)
    turn_cos = (
        twist_cos[:, :, None] * final_cos[None] - twist_sin[:, :, None] * final_sin[None]
    )
    turn_sin = (
        twist_sin[:, :, None] * final_cos[None] + twist_cos[:, :, None] * final_sin[None]
    )
    turn_table = lax.optimization_barrier(
        jnp.concatenate([turn_cos, -turn_sin, -turn_sin, -turn_cos], axis=1)
    )
    mode = (
        outer_len * jnp.arange(half_inner, dtype=jnp.int32)[:, None]
        + jnp.arange(outer_len, dtype=jnp.int32)[None, :]
    )
    paired_mode = jnp.concatenate([mode, mode], axis=1)[:, None, :]
    weights = jnp.where(paired_mode == 0, 1.0, 2.0).astype(jnp.float32) * spread
    slope_weights = weights * (16.0 * paired_mode.astype(jnp.float32) / total_modes)

    def exchange(blocks):
        return lax.all_to_all(blocks, AXES, split_axis=0, concat_axis=0, tiled=True)

    def stat_block(stats):
        flat = jnp.pad(stats.reshape(-1), (0, STAT_LANES - stats.size))
        return jnp.broadcast_to(flat, (group_size, rows, STAT_LANES))

    def read_stats(received, shape):
        flat = jnp.sum(received[:, 0, :], axis=0)
        return flat[: math.prod(shape)].reshape(shape)

    def to_points(coefs, stats):
        values = jnp.einsum("ni,brkn->ibrk", cheb_table, coefs, precision=PREC)
        blocks = values.reshape(group_size, rows, block_lanes)
        if stats is not None:
            blocks = jnp.concatenate([blocks, stat_block(stats)], axis=2)
        received = exchange(blocks)
        summed = None
        if stats is not None:
            summed = read_stats(received[:, :, block_lanes:], stats.shape)
            received = received[:, :, :block_lanes]
        spectrum = received.reshape(half_inner, split, rows, batch, 2, local_modes)
        spectrum = spectrum.transpose(0, 2, 3, 4, 1, 5).reshape(
            half_inner, fields, 2 * outer_len
        )

        def points_of(table, weighted):
            turned = jnp.einsum("sjq,qyl->jysl", table, weighted, precision=PREC)
            turned = turned.reshape(inner_len, fields, 4 * outer_len)
            return jnp.einsum("jyl,jlt->jyt", turned, turn_table, precision=PREC)

        values = points_of(value_table, spectrum * weights)
        slopes = points_of(slope_table, spectrum * slope_weights)
        return (values, slopes), summed

    def to_coefficients(points):
        turned = jnp.einsum("jyt,jlt->jyl", points, turn_table, precision=PREC) * gather_factor
        direct = turned[:, :, : 2 * outer_len].reshape(inner_len, -1)
        swapped = turned[:, :, 2 * outer_len :].reshape(inner_len, -1)
        spectrum = jnp.dot(back_cos, direct, precision=PREC) + jnp.dot(
            back_sin, swapped, precision=PREC
        )
        blocks = spectrum.reshape(half_inner, rows, batch, 2, split, local_modes)
        blocks = blocks.transpose(0, 4, 1, 2, 3, 5).reshape(group_size, rows, block_lanes)
        received = exchange(blocks).reshape(degrees, batch, 2, local_modes)
        return jnp.einsum("ibrk,ni->brkn", received, back_table, precision=PREC)

    def precondition(coefs):
        return jnp.einsum("kam,brkm->brka", taus, coefs, precision=PREC)

    def on_points(scale):
        return jnp.tile(scale, rows)[None, :, None]

    def on_coefs(scale):
        return scale[:, None, None, None]

    iterate = start
    kept_forcing = forcing * tau_keep
    base, nothing = to_points(iterate, None)
    for newton_step in range(NEWTON):
        base_points, base_slopes = base
        residual = iterate + precondition(
            to_coefficients(STRENGTH * base_points * base_slopes) - kept_forcing
        )
        local_square = jnp.sum(residual * residual, axis=(1, 2, 3))
        image, squared = to_points(residual, local_square)
        beta_norm = jnp.sqrt(squared)
        krylov_basis = [-residual / on_coefs(beta_norm)]
        images = [tuple(-part / on_points(beta_norm) for part in image)]
        hessen = []
        for column in range(KRYLOV):
            probe_points, probe_slopes = images[column]
            product = STRENGTH * (base_points * probe_slopes + probe_points * base_slopes)
            applied = krylov_basis[column] + precondition(to_coefficients(product))
            local_stats = jnp.stack(
                [jnp.sum(vector * applied, axis=(1, 2, 3)) for vector in krylov_basis + [applied]],
                axis=1,
            )
            last = column == KRYLOV - 1
            if last:
                stats = read_stats(exchange(stat_block(local_stats)), local_stats.shape)
            else:
                image, stats = to_points(applied, local_stats)
            projections, square = stats[:, :-1], stats[:, -1]
            length = jnp.sqrt(square - jnp.sum(projections * projections, axis=1))
            hessen.append(jnp.concatenate([projections, length[:, None]], axis=1))
            if not last:
                for index in range(column + 1):
                    applied = applied - on_coefs(projections[:, index]) * krylov_basis[index]
                    image = tuple(
                        part - on_points(projections[:, index]) * known
                        for part, known in zip(image, images[index])
                    )
                krylov_basis.append(applied / on_coefs(length))
                images.append(tuple(part / on_points(length) for part in image))
        solved = least_squares(hessen, beta_norm)
        for column in range(KRYLOV):
            iterate = iterate + on_coefs(solved[column]) * krylov_basis[column]
            base = tuple(
                part + on_points(solved[column]) * known
                for part, known in zip(base, images[column])
            )
    return iterate


def solution(mesh):
    return jax.shard_map(
        shards,
        mesh=mesh,
        in_specs=(
            P(None, None, ("modes", "cheb"), None),
            P(None, None, ("modes", "cheb"), None),
            P(("modes", "cheb"), None, None),
        ),
        out_specs=P(None, None, ("modes", "cheb"), None),
        check_vma=False,
    )
```
